32 devices in a mesh: dp: 4 (over y, z), tp: 8 (over x, core).
Axes of the slice: x: 4, y: 2, z: 2, core: 2. Of those that a mesh axis runs over, the one named last changes fastest.
The devices are a block of a 4x4x8 slice.
Arguments:
- x: bfloat16 [8, 2048, 4096], P('dp'), parts along dimension 0
- gamma: float32 [4096], replicated
- beta: float32 [4096], replicated
- wqkv: bfloat16 [4096, 12288], P(None, 'tp')
- wo: bfloat16 [16, 256, 4096], P('tp')
- w1: bfloat16 [4096, 16384], P(None, 'tp')
- w2: bfloat16 [16384, 4096], P('tp')
Outputs:
- output: bfloat16 [8, 2048, 4096], P('dp'), parts along dimension 0
There are 4 independent parts. The reference program is written for one: setup_inputs(seed, part) draws one part's arguments, and reference() takes and returns one part's arrays. A program takes and returns all parts, laid end to end along the dimension named above; an argument that names none is the same for every part.
All inputs are finite; a program needn't handle non-finite values.
Results may differ from the reference program's by a relative error of at most 0.0104537.
Values are sent between devices in bfloat16 or wider.
A program may use at most 768 MiB of HBM per device.

```python
import jax
import jax.numpy as jnp
from jax import lax

B = 2
S = 2048
D = 4096
HEADS = 16
KV = 16
HEAD = 256
FF = 16384


def setup_inputs(seed: int = 0, part: int = 0) -> dict:
    key = jax.random.key(seed)
    kx = jax.random.fold_in(jax.random.fold_in(key, 1), part)
    ks = jax.random.split(jax.random.fold_in(key, 2), 6)
    x = jax.random.normal(kx, (B, S, D), jnp.float32).astype(jnp.bfloat16)
    gamma = 1.0 + 0.3 * jax.random.normal(ks[0], (D,), jnp.float32)
    beta = 0.2 * jax.random.normal(ks[1], (D,), jnp.float32)
    wqkv = jax.random.normal(ks[2], (D, (HEADS + 2 * KV) * HEAD), jnp.float32) * D ** -0.5
    wo = jax.random.normal(ks[3], (HEADS, HEAD, D), jnp.float32) * ((HEADS * HEAD) ** -0.5 * 0.5 * S ** 0.25)
    w1 = jax.random.normal(ks[4], (D, FF), jnp.float32) * D ** -0.5
    w2 = jax.random.normal(ks[5], (FF, D), jnp.float32) * (0.7 * FF ** -0.5)
    return {'x': x, 'gamma': gamma, 'beta': beta,
            'wqkv': wqkv.astype(jnp.bfloat16), 'wo': wo.astype(jnp.bfloat16),
            'w1': w1.astype(jnp.bfloat16), 'w2': w2.astype(jnp.bfloat16)}


def layer_norm(x, gamma, beta):
    xf = x.astype(jnp.float32)
    mu = jnp.mean(xf, axis=-1, keepdims=True)
    var = jnp.mean(jnp.square(xf - mu), axis=-1, keepdims=True)
    return ((xf - mu) * lax.rsqrt(var + 1e-5) * gamma + beta).astype(jnp.bfloat16)


def reference(x, gamma, beta, wqkv, wo, w1, w2):
    hpg = HEADS // KV
    ntok = B * S
    ln = layer_norm(x, gamma, beta).reshape(ntok, D)
    qkv = jnp.dot(ln, wqkv, preferred_element_type=jnp.float32).astype(jnp.bfloat16)
    qkv = qkv.reshape(B, S, KV, hpg + 2, HEAD)
    pos = jnp.arange(S)
    causal = pos[:, None] >= pos[None, :]
    scale = HEAD ** -0.5

    def one_group(args):
        q, k, v = args
        sc = jnp.einsum('shd,td->hst', q.astype(jnp.float32), k.astype(jnp.float32)) * scale
        sc = jnp.where(causal[None], sc, -1e30)
        p = jax.nn.softmax(sc, axis=-1).astype(jnp.bfloat16)
        o = jnp.einsum('hst,td->shd', p.astype(jnp.float32), v.astype(jnp.float32))
        return o.astype(jnp.bfloat16)

    def one_seq(qkv_b):
        g = jnp.moveaxis(qkv_b, 1, 0)
        o = lax.map(one_group, (g[:, :, :hpg], g[:, :, hpg], g[:, :, hpg + 1]))
        return jnp.moveaxis(o, 0, 1).reshape(S, HEADS * HEAD)

    o = lax.map(one_seq, qkv).reshape(ntok, HEADS * HEAD)
    a = jnp.dot(o, wo.reshape(HEADS * HEAD, D), preferred_element_type=jnp.float32)
    hmid = jax.nn.gelu(jnp.dot(ln, w1, preferred_element_type=jnp.float32), approximate=False).astype(jnp.bfloat16)
    m = jnp.dot(hmid, w2, preferred_element_type=jnp.float32)
    upd = (a + m).astype(jnp.bfloat16).astype(jnp.float32).reshape(B, S, D)
    return (x.astype(jnp.float32) + upd).astype(jnp.bfloat16)
```

```python
import functools

import jax
import jax.numpy as jnp
from jax import lax
from jax.experimental import pallas as pl
from jax.experimental.pallas import tpu as pltpu
from jax.sharding import PartitionSpec as P

MESH = pl.DeviceIdType.MESH
F32 = jnp.float32
BF16 = jnp.bfloat16
BT = 512
NT = 512
NSLOT = 3
LOG2E = 1.4426950408889634


def dot(a, b):
    return jnp.dot(a, b, preferred_element_type=F32)


def gelu(x):
    return 0.5 * x * (1.0 + lax.erf(x * 0.7071067811865476))


def kernel(tp, seq, heads, dh,
           x, gamma, beta, wqkv, wo, w1, w2, y,
           wbuf, xbuf, ln, qkv, sc, h, pt, pr, cs, own, rs, relay, yt, xt, mx, acc,
           wsem, wosem, xsem, xtsem, ysem, psend, precv, ssem, rsem):
    t = lax.axis_index('tp')
    nx = tp // 2
    d, c = t // 2, t % 2
    left = lax.rem(d + nx - 1, nx)
    right = lax.rem(d + 1, nx)
    opp = lax.rem(d + 2, nx)
    partner = {'tp': d * 2 + (1 - c)}
    dev_l = {'tp': left * 2 + c}
    dev_r = {'tp': right * 2 + c}

    ntok, dm = x.shape
    nb = ntok // BT
    jb = seq // BT
    hw = heads * dh
    ff = w1.shape[1]
    nq = wqkv.shape[1] // NT
    nf = ff // NT
    hb = BT // 2
    LR = BT // (2 * nx)
    sub = NT // 2

    def tile(cc, o):
        return pl.multiple_of((cc * nx + o) * NT, NT)

    def ds_rows(b, off=0, n=BT):
        return pl.ds(pl.multiple_of(b * BT + off, hb), n)

    def w_q(i, slot):
        return [pltpu.make_async_copy(wqkv.at[:, pl.ds(pl.multiple_of(i * NT, NT), NT)], wbuf.at[slot], wsem.at[slot])]

    def w_f(i, slot):
        return [pltpu.make_async_copy(w1.at[:, pl.ds(pl.multiple_of(i * NT, NT), NT)], wbuf.at[slot], wsem.at[slot])]

    def owner(k):
        if isinstance(k, int):
            return (opp, right, left, d)[k]
        return lax.rem(d + jnp.where(k == 2, nx - 1, jnp.where(k == 3, 0, 2 - k)), nx)

    def w_o(cc, k, slot):
        col = tile(cc, owner(k))
        return [pltpu.make_async_copy(w2.at[:, pl.ds(col, NT)], wbuf.at[slot, pl.ds(0, ff)], wsem.at[slot]),
                pltpu.make_async_copy(wo.at[:, pl.ds(col, NT)], wbuf.at[slot, pl.ds(ff, hw)], wosem.at[slot])]

    def start(copies):
        for cp in copies:
            cp.start()

    def wait(copies):
        for cp in copies:
            cp.wait()

    def rc(i, src, dst, dev):
        return pltpu.make_async_remote_copy(src_ref=src, dst_ref=dst, send_sem=ssem.at[i], recv_sem=rsem.at[i],
                                            device_id=dev, device_id_type=MESH)

    rows_a, rows_b = pl.ds(0, hb), pl.ds(hb, hb)
    rs_opp_r = rc(0, cs.at[0, rows_b], relay.at[0], dev_r)
    rs_opp_l = rc(1, cs.at[0, rows_a], relay.at[1], dev_l)
    rs_dir_r = rc(2, cs.at[1, rows_a], rs.at[0], dev_r)
    rs_dir_l = rc(3, cs.at[2, rows_b], rs.at[1], dev_l)
    rs_cmb_r = rc(4, cs.at[1, rows_b], rs.at[2], dev_r)
    rs_cmb_l = rc(5, cs.at[2, rows_a], rs.at[3], dev_l)

    def ag_own(b):
        dst = y.at[ds_rows(b), pl.ds(tile(c, d), NT)]
        return rc(6, yt, dst, dev_r), rc(7, yt, dst, dev_l), rc(8, yt, dst, partner)

    def ag_own_arrived(b):
        def at(i, cc, o, dev):
            ref = y.at[ds_rows(b), pl.ds(tile(cc, o), NT)]
            return rc(i, yt, ref, dev)
        return at(6, c, left, dev_r), at(7, c, right, dev_l), at(8, 1 - c, d, partner)

    def y_tile(b, cc, o, off, n):
        return y.at[ds_rows(b, off, n), pl.ds(tile(cc, o), NT)]

    def ag_fwd(b):
        fb = y_tile(b, c, left, hb, hb)
        fa = y_tile(b, c, right, 0, hb)
        tl = y_tile(b, c, left, 0, BT)
        tr = y_tile(b, c, right, 0, BT)
        return (rc(9, fb, fb, dev_r), rc(10, fa, fa, dev_l), rc(11, tl, tl, partner), rc(12, tr, tr, partner))

    def ag_fwd_arrived(b):
        fb = y_tile(b, c, opp, hb, hb)
        fa = y_tile(b, c, opp, 0, hb)
        tl = y_tile(b, 1 - c, left, 0, BT)
        tr = y_tile(b, 1 - c, right, 0, BT)
        return (rc(9, fb, fb, dev_r), rc(10, fa, fa, dev_l), rc(11, tl, tl, partner), rc(12, tr, tr, partner))

    def ag_opp(b, cc):
        ref = y_tile(b, cc, opp, 0, BT)
        return rc(13, ref, ref, partner)

    def ptile(k):
        return pltpu.make_async_remote_copy(src_ref=pt.at[k], dst_ref=pr.at[k], send_sem=psend.at[k],
                                            recv_sem=precv.at[k], device_id=partner, device_id_type=MESH)

    def xt_copy(b):
        return pltpu.make_async_copy(x.at[ds_rows(b), pl.ds(tile(c, d), NT)], xt, xtsem)

    def yt_copy(b):
        return pltpu.make_async_copy(yt, y.at[ds_rows(b), pl.ds(tile(c, d), NT)], ysem)

    def x_copy(b):
        return pltpu.make_async_copy(x.at[ds_rows(b)], xbuf, xsem)

    def layer_norm(r0, n):
        for i in range(n // 16):
            r = pl.ds(pl.multiple_of(r0 + i * 16, 16), 16)
            v = xbuf[r, :].astype(F32)
            mu = jnp.sum(v, axis=-1, keepdims=True) * (1.0 / dm)
            v = v - mu
            var = jnp.sum(v * v, axis=-1, keepdims=True) * (1.0 / dm)
            ln[r, :] = (v * lax.rsqrt(var + 1e-5) * gamma[...] + beta[...]).astype(BF16)

    def t1():
        rs_opp_r.wait_recv()
        rs_opp_l.wait_recv()
        cs[1, hb:, :] = (cs[1, hb:, :].astype(F32) + relay[0].astype(F32)).astype(BF16)
        cs[2, :hb, :] = (cs[2, :hb, :].astype(F32) + relay[1].astype(F32)).astype(BF16)

    def t1_send():
        rs_cmb_r.start()
        rs_cmb_l.start()

    def t2(b):
        rs_dir_r.wait_recv()
        rs_dir_l.wait_recv()
        rs_cmb_r.wait_recv()
        rs_cmb_l.wait_recv()
        xt_copy(b).wait()

        def rows(r, p, q):
            tot = own[r, :] + (rs[p].astype(F32) + rs[q].astype(F32))
            yt[r, :] = (xt[r, :].astype(F32) + tot.astype(BF16).astype(F32)).astype(BF16)
        rows(slice(0, hb), 0, 3)
        rows(slice(hb, BT), 1, 2)

    def t3(b):
        for cp in ag_own(b):
            cp.start()
        yt_copy(b).start()

    def t4(b):
        al, ar, _ = ag_own_arrived(b)
        al.wait_recv()
        ar.wait_recv()
        for cp in ag_fwd(b):
            cp.start()
        for cp in (rs_opp_r, rs_opp_l, rs_dir_r, rs_dir_l, rs_cmb_r, rs_cmb_l):
            cp.wait_send()

    def t4_partner(b):
        ag_own_arrived(b)[2].wait_recv()
        for k in range(nx):
            ptile(k).wait_send()

    def t5(b):
        fb, fa, _, _ = ag_fwd_arrived(b)
        fb.wait_recv()
        fa.wait_recv()
        ag_opp(b, c).start()
        for cp in ag_own(b):
            cp.wait_send()
        yt_copy(b).wait()

    def t6(b):
        _, _, tl, tr = ag_fwd_arrived(b)
        tl.wait_recv()
        tr.wait_recv()
        ag_opp(b, 1 - c).wait_recv()
        for cp in ag_fwd(b):
            cp.wait_send()
        ag_opp(b, c).wait_send()

    start(w_q(0, 0))
    start(w_q(1, 1))
    x_copy(0).start()
    bar = pltpu.get_barrier_semaphore()
    for dev in (dev_l, dev_r, partner):
        pl.semaphore_signal(bar, inc=1, device_id=dev, device_id_type=MESH)
    x_copy(0).wait()

    @pl.loop(0, 2 * nx)
    def _(i):
        layer_norm(i * LR, LR)

    pl.semaphore_wait(bar, 3)

    def attention(j):
        scale = (dh ** -0.5) * LOG2E
        qr = pl.ds(pl.multiple_of(j * BT, BT), BT)
        for g in range(heads):
            q0, k0, v0 = g * 3 * dh, g * 3 * dh + dh, g * 3 * dh + 2 * dh
            q = qkv[qr, q0:q0 + dh]

            def lanes(s):
                m = s[:, :128]
                for n in range(1, BT // 128):
                    m = jnp.maximum(m, s[:, n * 128:(n + 1) * 128])
                return m

            def scores(kc):
                kr = pl.ds(pl.multiple_of(kc * BT, BT), BT)
                return lax.dot_general(q, qkv[kr, k0:k0 + dh], (((1,), (1,)), ((), ())), preferred_element_type=F32)

            s = scores(j)
            keep = lax.broadcasted_iota(jnp.int32, (BT, BT), 0) >= lax.broadcasted_iota(jnp.int32, (BT, BT), 1)
            s = jnp.where(keep, s, -1e30)
            sc[j] = s
            mx[...] = lanes(s)

            @pl.loop(0, j)
            def _(kc):
                s = scores(kc)
                sc[kc] = s
                mx[...] = jnp.maximum(mx[...], lanes(s))

            m = jnp.max(mx[...], axis=1, keepdims=True)
            mx[...] = jnp.zeros_like(mx)

            @pl.loop(0, j + 1)
            def _(kc):
                e = jnp.exp2((sc[kc] - m) * scale)
                sc[kc] = e
                a = e[:, :128]
                for n in range(1, BT // 128):
                    a = a + e[:, n * 128:(n + 1) * 128]
                mx[...] += a

            r = 1.0 / jnp.sum(mx[...], axis=1, keepdims=True)

            def pv(kc):
                kr = pl.ds(pl.multiple_of(kc * BT, BT), BT)
                return dot((sc[kc] * r).astype(BF16), qkv[kr, v0:v0 + dh])

            acc[...] = pv(0)

            @pl.loop(1, j + 1)
            def _(kc):
                acc[...] += pv(kc)

            h[:, ff + g * dh:ff + (g + 1) * dh] = acc[...].astype(BF16)

    @pl.loop(0, nb)
    def _(b):
        j = lax.rem(b, jb)
        rows = pl.ds(pl.multiple_of(j * BT, BT), BT)

        @pl.loop(0, nq)
        def _(i):
            slot = lax.rem(i, NSLOT)
            wait(w_q(i, slot))

            @pl.when(i == 0)
            def _():
                start(w_q(2, 2))

                @pl.when(b + 1 < nb)
                def _():
                    x_copy(b + 1).start()

            @pl.when(i > 0)
            def _():
                start(w_f(i - 1, lax.rem(i - 1, NSLOT)))

            qkv[rows, pl.ds(pl.multiple_of(i * NT, NT), NT)] = dot(ln[...], wbuf[slot]).astype(BF16)

            @pl.when((i == 0) & (b > 1))
            def _():
                t5(b - 2)

            @pl.when((i == 1) & (b > 1))
            def _():
                t6(b - 2)

            @pl.when((i == 2) & (b > 0))
            def _():
                t1()

        @pl.when(b > 0)
        def _():
            xt_copy(b - 1).start()
            t1_send()

        attention(j)

        @pl.loop(0, nf)
        def _(i):
            slot = lax.rem(i, NSLOT)
            wait(w_f(i, slot))

            @pl.when(i < 2)
            def _():
                start(w_f(i + 2, lax.rem(i + 2, NSLOT)))

            @pl.when(i >= 2)
            def _():
                start(w_o(1 - c, i - 2, lax.rem(i + 2, NSLOT)))

            for n in range(2):
                g = gelu(dot(ln[...], wbuf[slot, :, n * sub:(n + 1) * sub]))
                h[:, pl.ds(pl.multiple_of(i * NT + n * sub, sub), sub)] = g.astype(BF16)

            @pl.when((i == 0) & (b > 0))
            def _():
                t2(b - 1)

            @pl.when((i == 1) & (b > 0))
            def _():
                t3(b - 1)

            @pl.when((i == nf - 1) & (b > 0))
            def _():
                t4_partner(b - 1)

        @pl.when(b + 1 < nb)
        def _():
            x_copy(b + 1).wait()

        @pl.loop(0, nx)
        def _(k):
            i = k + nq + nf
            slot = lax.rem(i, NSLOT)
            wait(w_o(1 - c, k, slot))

            @pl.when(k < 2)
            def _():
                start(w_o(1 - c, k + 2, lax.rem(i + 2, NSLOT)))

            @pl.when(k >= 2)
            def _():
                start(w_o(c, k - 2, lax.rem(i + 2, NSLOT)))

            pt[k] = dot(h[...], wbuf[slot, :ff + hw, :]).astype(BF16)
            layer_norm(k * LR, LR)

            @pl.when(k > 0)
            def _():
                ptile(k - 1).start()

            @pl.when((k == 3) & (b > 0))
            def _():
                t4(b - 1)

        for k in range(nx):
            i = nq + nf + nx + k
            slot = i % NSLOT
            wait(w_o(c, k, slot))
            if k < 2:
                start(w_o(c, k + 2, (i + 2) % NSLOT))
            else:
                @pl.when(b + 1 < nb)
                def _():
                    start(w_q(k - 2, (i + 2) % NSLOT))
            if k == 0:
                own[...] = dot(h[...], wbuf[slot, :ff + hw, :])
                layer_norm((nx + k) * LR, LR)
                ptile(nx - 1).start()
                ptile(0).wait_recv()
                cs[0] = (own[...] + pr[0].astype(F32)).astype(BF16)
            else:
                ptile(k).wait_recv()
                s = dot(h[...], wbuf[slot, :ff + hw, :]) + pr[k].astype(F32)
                layer_norm((nx + k) * LR, LR)
                if k < nx - 1:
                    cs[k] = s.astype(BF16)
                else:
                    own[...] = s
            if k == 1:
                rs_opp_r.start()
                rs_opp_l.start()
            if k == 2:
                rs_dir_r.start()
            if k == 3:
                rs_dir_l.start()

    last = nb - 1
    xt_copy(last).start()
    t1()
    t5(last - 1)
    t1_send()
    t6(last - 1)
    t2(last)
    t3(last)
    t4_partner(last)
    t4(last)
    t5(last)
    t6(last)


def solution(mesh):
    tp = mesh.shape['tp']

    def local(x, gamma, beta, wqkv, wo, w1, w2):
        b, s, d = x.shape
        hl, dh, _ = wo.shape
        ff = w1.shape[1]
        nx = tp // 2
        ntok = b * s
        hb = BT // 2
        any_ = pl.BlockSpec(memory_space=pl.ANY)
        vm = pl.BlockSpec(memory_space=pltpu.VMEM)
        dma = pltpu.SemaphoreType.DMA
        flops = 2 * ntok * d * (wqkv.shape[1] + 2 * ff + hl * dh)
        out = pl.pallas_call(
            functools.partial(kernel, tp, s, hl, dh),
            out_shape=jax.ShapeDtypeStruct((ntok, d), BF16),
            in_specs=[any_, vm, vm, any_, any_, any_, any_],
            out_specs=any_,
            scratch_shapes=[
                pltpu.VMEM((NSLOT, d, NT), BF16),
                pltpu.VMEM((BT, d), BF16),
                pltpu.VMEM((BT, d), BF16),
                pltpu.VMEM((s, wqkv.shape[1]), BF16),
                pltpu.VMEM((s // BT, BT, BT), F32),
                pltpu.VMEM((BT, ff + hl * dh), BF16),
                pltpu.VMEM((nx, BT, NT), BF16),
                pltpu.VMEM((nx, BT, NT), BF16),
                pltpu.VMEM((nx - 1, BT, NT), BF16),
                pltpu.VMEM((BT, NT), F32),
                pltpu.VMEM((4, hb, NT), BF16),
                pltpu.VMEM((2, hb, NT), BF16),
                pltpu.VMEM((BT, NT), BF16),
                pltpu.VMEM((BT, NT), BF16),
                pltpu.VMEM((BT, 128), F32),
                pltpu.VMEM((BT, dh), F32),
                dma((NSLOT,)), dma((NSLOT,)), dma, dma, dma,
                dma((nx,)), dma((nx,)), dma((14,)), dma((14,)),
            ],
            compiler_params=pltpu.CompilerParams(collective_id=0, has_side_effects=True,
                                                 vmem_limit_bytes=67043328),
            cost_estimate=pl.CostEstimate(flops=flops, bytes_accessed=8 * 2 * (w1.size * 2 + wqkv.size + wo.size),
                                          transcendentals=0),
        )(x.reshape(ntok, d), gamma.reshape(1, d), beta.reshape(1, d), wqkv, wo.reshape(hl * dh, d), w1, w2)
        return out.reshape(b, s, d)

    return jax.shard_map(local, mesh=mesh,
                         in_specs=(P('dp', None, None), P(None), P(None), P(None, 'tp'),
                                   P('tp', None, None), P(None, 'tp'), P('tp', None)),
                         out_specs=P('dp', None, None), check_vma=False)
```

```python
import functools

import jax
import jax.numpy as jnp
from jax import lax
from jax.experimental import pallas as pl
from jax.experimental.pallas import tpu as pltpu
from jax.sharding import PartitionSpec as P

MESH = pl.DeviceIdType.MESH
F32 = jnp.float32
BF16 = jnp.bfloat16
BT = 512
NT = 512
NSLOT = 4
NKIND = 14
T2STEP = 3
LOG2E = 1.4426950408889634


def dot(a, b):
    return jnp.dot(a, b, preferred_element_type=F32)


def gelu(x):
    return 0.5 * x * (1.0 + lax.erf(x * 0.7071067811865476))


def kernel(tp, seq, heads, dh,
           x, gamma, beta, wqkv, wo, w1, w2, y,
           wbuf, xbuf, ln, qkv, sc, h, pt, pr, cs, own, rs, relay, yt, xt, mx, ls, acc,
           wsem, wosem, xsem, xtsem, ysem, psend, precv, ssem, rsem):
    t = lax.axis_index('tp')
    nx = tp // 2
    d, c = t // 2, t % 2
    left = lax.rem(d + nx - 1, nx)
    right = lax.rem(d + 1, nx)
    opp = lax.rem(d + 2, nx)
    partner = {'tp': d * 2 + (1 - c)}
    dev_l = {'tp': left * 2 + c}
    dev_r = {'tp': right * 2 + c}

    ntok, dm = x.shape
    nb = ntok // BT
    jb = seq // BT
    hw = heads * dh
    ff = w1.shape[1]
    nq = wqkv.shape[1] // NT
    nf = ff // NT
    hb = BT // 2
    LR = BT // (2 * nx)
    sub = NT // 2

    def tile(cc, o):
        return pl.multiple_of((cc * nx + o) * NT, NT)

    def ds_rows(b, off=0, n=BT):
        return pl.ds(pl.multiple_of(b * BT + off, hb), n)

    def w_q(i, slot):
        return [pltpu.make_async_copy(wqkv.at[:, pl.ds(pl.multiple_of(i * NT, NT), NT)], wbuf.at[slot], wsem.at[slot])]

    def w_f(i, slot):
        return [pltpu.make_async_copy(w1.at[:, pl.ds(pl.multiple_of(i * NT, NT), NT)], wbuf.at[slot], wsem.at[slot])]

    owners = (opp, right, left, d)

    def w_o(cc, k, slot):
        col = tile(cc, owners[k])
        return [pltpu.make_async_copy(w2.at[:, pl.ds(col, NT)], wbuf.at[slot, pl.ds(0, ff)], wsem.at[slot]),
                pltpu.make_async_copy(wo.at[:, pl.ds(col, NT)], wbuf.at[slot, pl.ds(ff, hw)], wosem.at[slot])]

    def loads(step):
        o = 2 * (step % 2)
        if step == 0:
            return w_q(0, o) + w_q(1, o + 1)
        if step == 1:
            return w_q(2, o)
        if step < 4:
            n = 2 * (step - 2)
            return w_f(n, o) + w_f(n + 1, o + 1)
        n = 2 * (step % 2)
        cc = 1 - c if step < 6 else c
        return w_o(cc, n, o) + w_o(cc, n + 1, o + 1)

    def start(copies):
        for cp in copies:
            cp.start()

    def wait(copies):
        for cp in copies:
            cp.wait()

    def par(b):
        return b % 2 if isinstance(b, int) else lax.rem(b, 2)

    def rc(i, b, src, dst, dev):
        n = i + NKIND * par(b)
        return pltpu.make_async_remote_copy(src_ref=src, dst_ref=dst, send_sem=ssem.at[n], recv_sem=rsem.at[n],
                                            device_id=dev, device_id_type=MESH)

    rows_a, rows_b = pl.ds(0, hb), pl.ds(hb, hb)

    def rs_opp(b):
        return rc(0, b, cs.at[0, rows_b], relay.at[0], dev_r), rc(1, b, cs.at[0, rows_a], relay.at[1], dev_l)

    def rs_dir_r(b):
        return rc(2, b, cs.at[1, rows_a], rs.at[4 * par(b)], dev_r)

    def rs_dir_l(b):
        return rc(3, b, cs.at[2, rows_b], rs.at[4 * par(b) + 1], dev_l)

    def rs_cmb(b):
        return (rc(4, b, cs.at[1, rows_b], rs.at[4 * par(b) + 2], dev_r),
                rc(5, b, cs.at[2, rows_a], rs.at[4 * par(b) + 3], dev_l))

    def y_tile(b, cc, o, off, n):
        return y.at[ds_rows(b, off, n), pl.ds(tile(cc, o), NT)]

    def ag_own(b):
        dst = y_tile(b, c, d, 0, BT)
        return [rc(6, b, yt, dst, dev_r), rc(7, b, yt, dst, dev_l), rc(8, b, yt, dst, partner)]

    def ag_own_l(b):
        return rc(6, b, yt, y_tile(b, c, left, 0, BT), dev_r)

    def ag_own_r(b):
        return rc(7, b, yt, y_tile(b, c, right, 0, BT), dev_l)

    def ag_own_p(b):
        return rc(8, b, yt, y_tile(b, 1 - c, d, 0, BT), partner)

    def fwd_b(b, o):
        ref = y_tile(b, c, o, hb, hb)
        return rc(9, b, ref, ref, dev_r)

    def fwd_a(b, o):
        ref = y_tile(b, c, o, 0, hb)
        return rc(10, b, ref, ref, dev_l)

    def to_partner(i, b, cc, o):
        ref = y_tile(b, cc, o, 0, BT)
        return rc(i, b, ref, ref, partner)

    def ag_fwd(b):
        return [fwd_b(b, left), fwd_a(b, right), to_partner(11, b, c, left), to_partner(12, b, c, right)]

    def ptile(k):
        return pltpu.make_async_remote_copy(src_ref=pt.at[k], dst_ref=pr.at[k], send_sem=psend.at[k],
                                            recv_sem=precv.at[k], device_id=partner, device_id_type=MESH)

    def xt_copy(b):
        return pltpu.make_async_copy(x.at[ds_rows(b), pl.ds(tile(c, d), NT)], xt, xtsem)

    def yt_copy(b):
        return pltpu.make_async_copy(yt, y.at[ds_rows(b), pl.ds(tile(c, d), NT)], ysem)

    def x_copy(b):
        return pltpu.make_async_copy(x.at[ds_rows(b)], xbuf, xsem)

    def layer_norm(r0, n):
        for i in range(n // 16):
            r = pl.ds(pl.multiple_of(r0 + i * 16, 16), 16)
            v = xbuf[r, :].astype(F32)
            mu = jnp.sum(v, axis=-1, keepdims=True) * (1.0 / dm)
            v = v - mu
            var = jnp.sum(v * v, axis=-1, keepdims=True) * (1.0 / dm)
            ln[r, :] = (v * lax.rsqrt(var + 1e-5) * gamma[...] + beta[...]).astype(BF16)

    def t1(b):
        for cp in rs_opp(b):
            cp.wait_recv()
        cs[1, hb:, :] = (cs[1, hb:, :].astype(F32) + relay[0].astype(F32)).astype(BF16)
        cs[2, :hb, :] = (cs[2, :hb, :].astype(F32) + relay[1].astype(F32)).astype(BF16)
        for k in range(nx):
            ptile(k).wait_send()

    def t1_send(b):
        start(rs_cmb(b))

    def t2(b):
        rs_dir_r(b).wait_recv()
        rs_dir_l(b).wait_recv()
        for cp in rs_cmb(b):
            cp.wait_recv()
        xt_copy(b).wait()
        n = 4 * par(b)

        def rows(r, p, q):
            tot = own[r, :] + (rs[n + p].astype(F32) + rs[n + q].astype(F32))
            yt[r, :] = (xt[r, :].astype(F32) + tot.astype(BF16).astype(F32)).astype(BF16)
        rows(slice(0, hb), 0, 3)
        rows(slice(hb, BT), 1, 2)

    def t3(b):
        start(ag_own(b))
        yt_copy(b).start()

    def rs_sent(b):
        for cp in (*rs_opp(b), rs_dir_r(b), rs_dir_l(b), *rs_cmb(b)):
            cp.wait_send()

    def t4_wait(b):
        ag_own_l(b).wait_recv()
        ag_own_r(b).wait_recv()

    def t4_send(b):
        start(ag_fwd(b))
        for cp in ag_own(b):
            cp.wait_send()
        yt_copy(b).wait()

    def t5(b):
        fwd_b(b, opp).wait_recv()
        fwd_a(b, opp).wait_recv()
        to_partner(13, b, c, opp).start()

    def t6(b):
        to_partner(11, b, 1 - c, left).wait_recv()
        to_partner(12, b, 1 - c, right).wait_recv()
        to_partner(13, b, 1 - c, opp).wait_recv()
        for cp in ag_fwd(b):
            cp.wait_send()
        to_partner(13, b, c, opp).wait_send()

    x_copy(0).start()
    start(loads(0))
    bar = pltpu.get_barrier_semaphore()
    for dev in (dev_l, dev_r, partner):
        pl.semaphore_signal(bar, inc=1, device_id=dev, device_id_type=MESH)
    x_copy(0).wait()

    @pl.loop(0, 2 * nx)
    def _(i):
        layer_norm(i * LR, LR)

    pl.semaphore_wait(bar, 3)

    nl = BT // 128

    def scores(j):
        qr = pl.ds(pl.multiple_of(j * BT, BT), BT)
        q0 = [g * 3 * dh for g in range(heads)]

        def lanes(s):
            m = s[:, :128]
            for n in range(1, nl):
                m = jnp.maximum(m, s[:, n * 128:(n + 1) * 128])
            return m

        def qk(g, kc):
            kr = pl.ds(pl.multiple_of(kc * BT, BT), BT)
            return lax.dot_general(qkv[qr, q0[g]:q0[g] + dh], qkv[kr, q0[g] + dh:q0[g] + 2 * dh],
                                   (((1,), (1,)), ((), ())), preferred_element_type=F32)

        keep = lax.broadcasted_iota(jnp.int32, (BT, BT), 0) >= lax.broadcasted_iota(jnp.int32, (BT, BT), 1)
        for g in range(heads):
            s = jnp.where(keep, qk(g, j), -1e30)
            sc[g, j] = s
            mx[g] = lanes(s)

        @pl.loop(0, j)
        def _(kc):
            for g in range(heads):
                s = qk(g, kc)
                sc[g, kc] = s
                mx[g] = jnp.maximum(mx[g], lanes(s))

        for g in range(heads):
            mx[g] = jnp.broadcast_to(jnp.max(mx[g], axis=1, keepdims=True), (BT, 128))
            ls[g] = jnp.zeros((BT, 128), F32)

    def exponentials(j):
        scale = (dh ** -0.5) * LOG2E

        @pl.loop(0, j + 1)
        def _(kc):
            for g in range(heads):
                m = mx[g]
                a = ls[g]
                for n in range(nl):
                    r = slice(n * 128, (n + 1) * 128)
                    e = jnp.exp2((sc[g, kc, :, r] - m) * scale)
                    sc[g, kc, :, r] = e
                    a = a + e
                ls[g] = a

    def values(j):
        for g in range(heads):
            r = 1.0 / jnp.sum(ls[g], axis=1, keepdims=True)
            ls[g] = jnp.broadcast_to(r, (BT, 128))

        def pv(g, kc):
            kr = pl.ds(pl.multiple_of(kc * BT, BT), BT)
            r = ls[g]
            p = jnp.concatenate([(sc[g, kc, :, n * 128:(n + 1) * 128] * r).astype(BF16) for n in range(nl)], axis=1)
            return dot(p, qkv[kr, g * 3 * dh + 2 * dh:(g + 1) * 3 * dh])

        for g in range(heads):
            acc[g] = pv(g, 0)

        @pl.loop(1, j + 1)
        def _(kc):
            for g in range(heads):
                acc[g] += pv(g, kc)

        for g in range(heads):
            h[:, ff + g * dh:ff + (g + 1) * dh] = acc[g].astype(BF16)

    @pl.loop(0, nb)
    def _(b):
        j = lax.rem(b, jb)
        rows = pl.ds(pl.multiple_of(j * BT, BT), BT)

        def begin(step):
            wait(loads(step))
            if step < 7:
                start(loads(step + 1))
            else:
                @pl.when(b + 1 < nb)
                def _():
                    start(loads(0))

        def w(step, n, depth=dm):
            return wbuf[2 * (step % 2) + n, :depth, :]

        begin(0)

        @pl.when(b > 0)
        def _():
            rs_dir_l(b - 1).start()
            xt_copy(b - 1).start()

        @pl.when(b + 1 < nb)
        def _():
            x_copy(b + 1).start()

        for n in range(2):
            qkv[rows, n * NT:(n + 1) * NT] = dot(ln[...], w(0, n)).astype(BF16)
        begin(1)
        qkv[rows, 2 * NT:3 * NT] = dot(ln[...], w(1, 0)).astype(BF16)

        @pl.when(b > 1)
        def _():
            t4_wait(b - 2)

        @pl.when(b > 0)
        def _():
            t1(b - 1)

        scores(j)

        @pl.when(b > 0)
        def _():
            t1_send(b - 1)

        @pl.when(b > 1)
        def _():
            t4_send(b - 2)

        exponentials(j)
        values(j)

        for step in (2, 3):
            begin(step)
            for n in range(2):
                i = 2 * (step - 2) + n
                h[:, i * NT:(i + 1) * NT] = gelu(dot(ln[...], w(step, n))).astype(BF16)
            if step == T2STEP:
                @pl.when(b > 0)
                def _():
                    t2(b - 1)

        @pl.when(b + 1 < nb)
        def _():
            x_copy(b + 1).wait()

        for step in (4, 5):
            begin(step)
            if step == 4:
                @pl.when(b > 0)
                def _():
                    t3(b - 1)
            else:
                @pl.when(b > 0)
                def _():
                    ag_own_p(b - 1).wait_recv()
                    rs_sent(b - 1)

                ptile(0).start()
                ptile(1).start()
            for n in range(2):
                pt[2 * (step - 4) + n] = dot(h[...], w(step, n, ff + hw)).astype(BF16)
                layer_norm((2 * (step - 4) + n) * LR, LR)

        @pl.when(b > 1)
        def _():
            t5(b - 2)

        begin(6)
        ptile(2).start()
        ptile(3).start()
        ptile(0).wait_recv()
        ptile(1).wait_recv()
        for n in range(2):
            cs[n] = (dot(h[...], w(6, n, ff + hw)) + pr[n].astype(F32)).astype(BF16)
            layer_norm((4 + n) * LR, LR)
        begin(7)
        start(rs_opp(b))
        rs_dir_r(b).start()
        ptile(2).wait_recv()
        ptile(3).wait_recv()
        cs[2] = (dot(h[...], w(7, 0, ff + hw)) + pr[2].astype(F32)).astype(BF16)
        layer_norm(6 * LR, LR)
        own[...] = dot(h[...], w(7, 1, ff + hw)) + pr[3].astype(F32)
        layer_norm(7 * LR, LR)

        @pl.when(b > 1)
        def _():
            t6(b - 2)

    last = nb - 1
    rs_dir_l(last).start()
    xt_copy(last).start()
    t4_wait(last - 1)
    t1(last)
    t1_send(last)
    t4_send(last - 1)
    t2(last)
    t3(last)
    t5(last - 1)
    ag_own_p(last).wait_recv()
    rs_sent(last)
    t6(last - 1)
    t4_wait(last)
    t4_send(last)
    t5(last)
    t6(last)


def solution(mesh):
    tp = mesh.shape['tp']

    def local(x, gamma, beta, wqkv, wo, w1, w2):
        b, s, d = x.shape
        hl, dh, _ = wo.shape
        ff = w1.shape[1]
        nx = tp // 2
        ntok = b * s
        hb = BT // 2
        any_ = pl.BlockSpec(memory_space=pl.ANY)
        vm = pl.BlockSpec(memory_space=pltpu.VMEM)
        dma = pltpu.SemaphoreType.DMA
        flops = 2 * ntok * d * (wqkv.shape[1] + 2 * ff + hl * dh)
        out = pl.pallas_call(
            functools.partial(kernel, tp, s, hl, dh),
            out_shape=jax.ShapeDtypeStruct((ntok, d), BF16),
            in_specs=[any_, vm, vm, any_, any_, any_, any_],
            out_specs=any_,
            scratch_shapes=[
                pltpu.VMEM((NSLOT, d, NT), BF16),
                pltpu.VMEM((BT, d), BF16),
                pltpu.VMEM((BT, d), BF16),
                pltpu.VMEM((s, wqkv.shape[1]), BF16),
                pltpu.VMEM((hl, s // BT, BT, BT), F32),
                pltpu.VMEM((BT, ff + hl * dh), BF16),
                pltpu.VMEM((nx, BT, NT), BF16),
                pltpu.VMEM((nx, BT, NT), BF16),
                pltpu.VMEM((nx - 1, BT, NT), BF16),
                pltpu.VMEM((BT, NT), F32),
                pltpu.VMEM((8, hb, NT), BF16),
                pltpu.VMEM((2, hb, NT), BF16),
                pltpu.VMEM((BT, NT), BF16),
                pltpu.VMEM((BT, NT), BF16),
                pltpu.VMEM((hl, BT, 128), F32),
                pltpu.VMEM((hl, BT, 128), F32),
                pltpu.VMEM((hl, BT, dh), F32),
                dma((NSLOT,)), dma((NSLOT,)), dma, dma, dma,
                dma((nx,)), dma((nx,)), dma((2 * NKIND,)), dma((2 * NKIND,)),
            ],
            compiler_params=pltpu.CompilerParams(collective_id=0, has_side_effects=True,
                                                 vmem_limit_bytes=67043328),
            cost_estimate=pl.CostEstimate(flops=flops, bytes_accessed=8 * 2 * (w1.size * 2 + wqkv.size + wo.size),
                                          transcendentals=0),
        )(x.reshape(ntok, d), gamma.reshape(1, d), beta.reshape(1, d), wqkv, wo.reshape(hl * dh, d), w1, w2)
        return out.reshape(b, s, d)

    return jax.shard_map(local, mesh=mesh,
                         in_specs=(P('dp', None, None), P(None), P(None), P(None, 'tp'),
                                   P('tp', None, None), P(None, 'tp'), P('tp', None)),
                         out_specs=P('dp', None, None), check_vma=False)
```

```python
import functools

import jax
import jax.numpy as jnp
from jax import lax
from jax.experimental import pallas as pl
from jax.experimental.pallas import tpu as pltpu
from jax.sharding import PartitionSpec as P

MESH = pl.DeviceIdType.MESH
F32 = jnp.float32
BF16 = jnp.bfloat16
BT = 512
NT = 512
NSLOT = 4
NKIND = 14
T2STEP = 3
LOG2E = 1.4426950408889634


def dot(a, b):
    return jnp.dot(a, b, preferred_element_type=F32)


def gelu(x):
    return 0.5 * x * (1.0 + lax.erf(x * 0.7071067811865476))


def kernel(tp, seq, heads, dh,
           x, gamma, beta, wqkv, wo, w1, w2, y,
           wbuf, xbuf, ln, qkv, sc, h, pt, pr, cs, own, rs, relay, yt, xt, mx, ls,
           wsem, wosem, xsem, xtsem, ysem, psend, precv, ssem, rsem):
    t = lax.axis_index('tp')
    nx = tp // 2
    d, c = t // 2, t % 2
    left = lax.rem(d + nx - 1, nx)
    right = lax.rem(d + 1, nx)
    opp = lax.rem(d + 2, nx)
    partner = {'tp': d * 2 + (1 - c)}
    dev_l = {'tp': left * 2 + c}
    dev_r = {'tp': right * 2 + c}

    ntok, dm = x.shape
    nb = ntok // BT
    jb = seq // BT
    hw = heads * dh
    ff = w1.shape[1]
    nq = wqkv.shape[1] // NT
    nf = ff // NT
    hb = BT // 2
    LR = BT // (2 * nx)
    sub = NT // 2

    def tile(cc, o):
        return pl.multiple_of((cc * nx + o) * NT, NT)

    def ds_rows(b, off=0, n=BT):
        return pl.ds(pl.multiple_of(b * BT + off, hb), n)

    def w_q(i, slot):
        return [pltpu.make_async_copy(wqkv.at[:, pl.ds(pl.multiple_of(i * NT, NT), NT)], wbuf.at[slot], wsem.at[slot])]

    def w_f(i, slot):
        return [pltpu.make_async_copy(w1.at[:, pl.ds(pl.multiple_of(i * NT, NT), NT)], wbuf.at[slot], wsem.at[slot])]

    owners = (opp, right, left, d)

    def w_o(cc, k, slot):
        col = tile(cc, owners[k])
        return [pltpu.make_async_copy(w2.at[:, pl.ds(col, NT)], wbuf.at[slot, pl.ds(0, ff)], wsem.at[slot]),
                pltpu.make_async_copy(wo.at[:, pl.ds(col, NT)], wbuf.at[slot, pl.ds(ff, hw)], wosem.at[slot])]

    def loads(step):
        o = 2 * (step % 2)
        if step == 0:
            return w_q(0, o) + w_q(1, o + 1)
        if step == 1:
            return w_q(2, o)
        if step < 4:
            n = 2 * (step - 2)
            return w_f(n, o) + w_f(n + 1, o + 1)
        n = 2 * (step % 2)
        cc = 1 - c if step < 6 else c
        return w_o(cc, n, o) + w_o(cc, n + 1, o + 1)

    def start(copies):
        for cp in copies:
            cp.start()

    def wait(copies):
        for cp in copies:
            cp.wait()

    def par(b):
        return b % 2 if isinstance(b, int) else lax.rem(b, 2)

    def rc(i, b, src, dst, dev):
        n = i + NKIND * par(b)
        return pltpu.make_async_remote_copy(src_ref=src, dst_ref=dst, send_sem=ssem.at[n], recv_sem=rsem.at[n],
                                            device_id=dev, device_id_type=MESH)

    rows_a, rows_b = pl.ds(0, hb), pl.ds(hb, hb)

    def rs_opp(b):
        return rc(0, b, cs.at[0, rows_b], relay.at[0], dev_r), rc(1, b, cs.at[0, rows_a], relay.at[1], dev_l)

    def rs_dir_r(b):
        return rc(2, b, cs.at[1, rows_a], rs.at[4 * par(b)], dev_r)

    def rs_dir_l(b):
        return rc(3, b, cs.at[2, rows_b], rs.at[4 * par(b) + 1], dev_l)

    def rs_cmb(b):
        return (rc(4, b, cs.at[1, rows_b], rs.at[4 * par(b) + 2], dev_r),
                rc(5, b, cs.at[2, rows_a], rs.at[4 * par(b) + 3], dev_l))

    def y_tile(b, cc, o, off, n):
        return y.at[ds_rows(b, off, n), pl.ds(tile(cc, o), NT)]

    def ag_own(b):
        dst = y_tile(b, c, d, 0, BT)
        return [rc(6, b, yt, dst, dev_r), rc(7, b, yt, dst, dev_l), rc(8, b, yt, dst, partner)]

    def ag_own_l(b):
        return rc(6, b, yt, y_tile(b, c, left, 0, BT), dev_r)

    def ag_own_r(b):
        return rc(7, b, yt, y_tile(b, c, right, 0, BT), dev_l)

    def ag_own_p(b):
        return rc(8, b, yt, y_tile(b, 1 - c, d, 0, BT), partner)

    def fwd_b(b, o):
        ref = y_tile(b, c, o, hb, hb)
        return rc(9, b, ref, ref, dev_r)

    def fwd_a(b, o):
        ref = y_tile(b, c, o, 0, hb)
        return rc(10, b, ref, ref, dev_l)

    def to_partner(i, b, cc, o):
        ref = y_tile(b, cc, o, 0, BT)
        return rc(i, b, ref, ref, partner)

    def ag_fwd(b):
        return [fwd_b(b, left), fwd_a(b, right), to_partner(11, b, c, left), to_partner(12, b, c, right)]

    def ptile(k):
        return pltpu.make_async_remote_copy(src_ref=pt.at[k], dst_ref=pr.at[k], send_sem=psend.at[k],
                                            recv_sem=precv.at[k], device_id=partner, device_id_type=MESH)

    def xt_copy(b):
        return pltpu.make_async_copy(x.at[ds_rows(b), pl.ds(tile(c, d), NT)], xt, xtsem)

    def yt_copy(b):
        return pltpu.make_async_copy(yt, y.at[ds_rows(b), pl.ds(tile(c, d), NT)], ysem)

    def x_copy(b):
        return pltpu.make_async_copy(x.at[ds_rows(b)], xbuf, xsem)

    def layer_norm(r0, n):
        for i in range(n // 16):
            r = pl.ds(pl.multiple_of(r0 + i * 16, 16), 16)
            v = xbuf[r, :].astype(F32)
            mu = jnp.sum(v, axis=-1, keepdims=True) * (1.0 / dm)
            v = v - mu
            var = jnp.sum(v * v, axis=-1, keepdims=True) * (1.0 / dm)
            ln[r, :] = (v * lax.rsqrt(var + 1e-5) * gamma[...] + beta[...]).astype(BF16)

    def t1(b):
        for cp in rs_opp(b):
            cp.wait_recv()
        cs[1, hb:, :] = (cs[1, hb:, :].astype(F32) + relay[0].astype(F32)).astype(BF16)
        cs[2, :hb, :] = (cs[2, :hb, :].astype(F32) + relay[1].astype(F32)).astype(BF16)
        for k in range(nx):
            ptile(k).wait_send()

    def t1_send(b):
        start(rs_cmb(b))

    def t2(b):
        rs_dir_r(b).wait_recv()
        rs_dir_l(b).wait_recv()
        for cp in rs_cmb(b):
            cp.wait_recv()
        xt_copy(b).wait()
        n = 4 * par(b)

        def rows(r, p, q):
            tot = own[r, :] + (rs[n + p].astype(F32) + rs[n + q].astype(F32))
            yt[r, :] = (xt[r, :].astype(F32) + tot.astype(BF16).astype(F32)).astype(BF16)
        rows(slice(0, hb), 0, 3)
        rows(slice(hb, BT), 1, 2)

    def t3(b):
        start(ag_own(b))
        yt_copy(b).start()

    def rs_sent(b):
        for cp in (*rs_opp(b), rs_dir_r(b), rs_dir_l(b), *rs_cmb(b)):
            cp.wait_send()

    def t4_wait(b):
        ag_own_l(b).wait_recv()
        ag_own_r(b).wait_recv()

    def t4_send(b):
        start(ag_fwd(b))
        for cp in ag_own(b):
            cp.wait_send()
        yt_copy(b).wait()

    def t5(b):
        fwd_b(b, opp).wait_recv()
        fwd_a(b, opp).wait_recv()
        to_partner(13, b, c, opp).start()

    def t6(b):
        to_partner(11, b, 1 - c, left).wait_recv()
        to_partner(12, b, 1 - c, right).wait_recv()
        to_partner(13, b, 1 - c, opp).wait_recv()
        for cp in ag_fwd(b):
            cp.wait_send()
        to_partner(13, b, c, opp).wait_send()

    x_copy(0).start()
    start(loads(0))
    bar = pltpu.get_barrier_semaphore()
    for dev in (dev_l, dev_r, partner):
        pl.semaphore_signal(bar, inc=1, device_id=dev, device_id_type=MESH)
    x_copy(0).wait()

    @pl.loop(0, 2 * nx)
    def _(i):
        layer_norm(i * LR, LR)

    pl.semaphore_wait(bar, 3)

    nl = BT // 128

    def scores(j):
        qr = slice(j * BT, (j + 1) * BT)
        q0 = [g * 3 * dh for g in range(heads)]

        def lanes(s):
            m = s[:, :128]
            for n in range(1, nl):
                m = jnp.maximum(m, s[:, n * 128:(n + 1) * 128])
            return m

        def qk(g, kc):
            kr = slice(kc * BT, (kc + 1) * BT)
            return lax.dot_general(qkv[qr, q0[g]:q0[g] + dh], qkv[kr, q0[g] + dh:q0[g] + 2 * dh],
                                   (((1,), (1,)), ((), ())), preferred_element_type=F32)

        keep = lax.broadcasted_iota(jnp.int32, (BT, BT), 0) >= lax.broadcasted_iota(jnp.int32, (BT, BT), 1)
        for g in range(heads):
            m = None
            for kc in range(j + 1):
                s = qk(g, kc)
                if kc == j:
                    s = jnp.where(keep, s, -1e30)
                sc[g, kc] = s
                m = lanes(s) if m is None else jnp.maximum(m, lanes(s))
            mx[g] = jnp.broadcast_to(jnp.max(m, axis=1, keepdims=True), (BT, 128))

    def values(j):
        scale = (dh ** -0.5) * LOG2E
        for g in range(heads):
            m = mx[g]
            a = None
            for kc in range(j + 1):
                for n in range(nl):
                    r = slice(n * 128, (n + 1) * 128)
                    e = jnp.exp2((sc[g, kc, :, r] - m) * scale)
                    sc[g, kc, :, r] = e
                    a = e if a is None else a + e
            ls[g] = jnp.broadcast_to(1.0 / jnp.sum(a, axis=1, keepdims=True), (BT, 128))
        for g in range(heads):
            r = ls[g]
            p = jnp.concatenate([(sc[g, kc, :, n * 128:(n + 1) * 128] * r).astype(BF16)
                                 for kc in range(j + 1) for n in range(nl)], axis=1)
            v0 = g * 3 * dh + 2 * dh
            h[:, ff + g * dh:ff + (g + 1) * dh] = dot(p, qkv[:(j + 1) * BT, v0:v0 + dh]).astype(BF16)

    def for_block(j, f):
        for n in range(jb):
            pl.when(j == n)(functools.partial(f, n))

    @pl.loop(0, nb)
    def _(b):
        j = lax.rem(b, jb)
        rows = pl.ds(pl.multiple_of(j * BT, BT), BT)

        def begin(step):
            wait(loads(step))
            if step < 7:
                start(loads(step + 1))
            else:
                @pl.when(b + 1 < nb)
                def _():
                    start(loads(0))

        def w(step, n, depth=dm):
            return wbuf[2 * (step % 2) + n, :depth, :]

        begin(0)

        @pl.when(b > 0)
        def _():
            rs_dir_l(b - 1).start()
            xt_copy(b - 1).start()

        @pl.when(b + 1 < nb)
        def _():
            x_copy(b + 1).start()

        for n in range(2):
            qkv[rows, n * NT:(n + 1) * NT] = dot(ln[...], w(0, n)).astype(BF16)
        begin(1)
        qkv[rows, 2 * NT:3 * NT] = dot(ln[...], w(1, 0)).astype(BF16)

        @pl.when(b > 1)
        def _():
            t4_wait(b - 2)

        @pl.when(b > 0)
        def _():
            t1(b - 1)

        for_block(j, scores)

        @pl.when(b > 0)
        def _():
            t1_send(b - 1)

        @pl.when(b > 1)
        def _():
            t4_send(b - 2)

        for_block(j, values)

        for step in (2, 3):
            begin(step)
            for n in range(2):
                i = 2 * (step - 2) + n
                h[:, i * NT:(i + 1) * NT] = gelu(dot(ln[...], w(step, n))).astype(BF16)
            if step == T2STEP:
                @pl.when(b > 0)
                def _():
                    t2(b - 1)

        @pl.when(b + 1 < nb)
        def _():
            x_copy(b + 1).wait()

        for step in (4, 5):
            begin(step)
            if step == 4:
                @pl.when(b > 0)
                def _():
                    t3(b - 1)
            else:
                @pl.when(b > 0)
                def _():
                    ag_own_p(b - 1).wait_recv()
                    rs_sent(b - 1)

                ptile(0).start()
                ptile(1).start()
            for n in range(2):
                pt[2 * (step - 4) + n] = dot(h[...], w(step, n, ff + hw)).astype(BF16)
                layer_norm((2 * (step - 4) + n) * LR, LR)

        @pl.when(b > 1)
        def _():
            t5(b - 2)

        begin(6)
        ptile(2).start()
        ptile(3).start()
        ptile(0).wait_recv()
        ptile(1).wait_recv()
        for n in range(2):
            cs[n] = (dot(h[...], w(6, n, ff + hw)) + pr[n].astype(F32)).astype(BF16)
            layer_norm((4 + n) * LR, LR)
        begin(7)
        start(rs_opp(b))
        rs_dir_r(b).start()
        ptile(2).wait_recv()
        ptile(3).wait_recv()
        cs[2] = (dot(h[...], w(7, 0, ff + hw)) + pr[2].astype(F32)).astype(BF16)
        layer_norm(6 * LR, LR)
        own[...] = dot(h[...], w(7, 1, ff + hw)) + pr[3].astype(F32)
        layer_norm(7 * LR, LR)

        @pl.when(b > 1)
        def _():
            t6(b - 2)

    last = nb - 1
    rs_dir_l(last).start()
    xt_copy(last).start()
    t4_wait(last - 1)
    t1(last)
    t1_send(last)
    t4_send(last - 1)
    t2(last)
    t3(last)
    t5(last - 1)
    ag_own_p(last).wait_recv()
    rs_sent(last)
    t6(last - 1)
    t4_wait(last)
    t4_send(last)
    t5(last)
    t6(last)


def solution(mesh):
    tp = mesh.shape['tp']

    def local(x, gamma, beta, wqkv, wo, w1, w2):
        b, s, d = x.shape
        hl, dh, _ = wo.shape
        ff = w1.shape[1]
        nx = tp // 2
        ntok = b * s
        hb = BT // 2
        any_ = pl.BlockSpec(memory_space=pl.ANY)
        vm = pl.BlockSpec(memory_space=pltpu.VMEM)
        dma = pltpu.SemaphoreType.DMA
        flops = 2 * ntok * d * (wqkv.shape[1] + 2 * ff + hl * dh)
        out = pl.pallas_call(
            functools.partial(kernel, tp, s, hl, dh),
            out_shape=jax.ShapeDtypeStruct((ntok, d), BF16),
            in_specs=[any_, vm, vm, any_, any_, any_, any_],
            out_specs=any_,
            scratch_shapes=[
                pltpu.VMEM((NSLOT, d, NT), BF16),
                pltpu.VMEM((BT, d), BF16),
                pltpu.VMEM((BT, d), BF16),
                pltpu.VMEM((s, wqkv.shape[1]), BF16),
                pltpu.VMEM((hl, s // BT, BT, BT), F32),
                pltpu.VMEM((BT, ff + hl * dh), BF16),
                pltpu.VMEM((nx, BT, NT), BF16),
                pltpu.VMEM((nx, BT, NT), BF16),
                pltpu.VMEM((nx - 1, BT, NT), BF16),
                pltpu.VMEM((BT, NT), F32),
                pltpu.VMEM((8, hb, NT), BF16),
                pltpu.VMEM((2, hb, NT), BF16),
                pltpu.VMEM((BT, NT), BF16),
                pltpu.VMEM((BT, NT), BF16),
                pltpu.VMEM((hl, BT, 128), F32),
                pltpu.VMEM((hl, BT, 128), F32),
                dma((NSLOT,)), dma((NSLOT,)), dma, dma, dma,
                dma((nx,)), dma((nx,)), dma((2 * NKIND,)), dma((2 * NKIND,)),
            ],
            compiler_params=pltpu.CompilerParams(collective_id=0, has_side_effects=True,
                                                 vmem_limit_bytes=67043328),
            cost_estimate=pl.CostEstimate(flops=flops, bytes_accessed=8 * 2 * (w1.size * 2 + wqkv.size + wo.size),
                                          transcendentals=0),
        )(x.reshape(ntok, d), gamma.reshape(1, d), beta.reshape(1, d), wqkv, wo.reshape(hl * dh, d), w1, w2)
        return out.reshape(b, s, d)

    return jax.shard_map(local, mesh=mesh,
                         in_specs=(P('dp', None, None), P(None), P(None), P(None, 'tp'),
                                   P('tp', None, None), P(None, 'tp'), P('tp', None)),
                         out_specs=P('dp', None, None), check_vma=False)
```
